16 devices in a mesh: rep: 2 (over y, z), fsdp: 8 (over x, core).
Axes of the slice: x: 4, y: 2, z: 1, core: 2. Of those that a mesh axis runs over, the one named last changes fastest.
The devices are a block of a 4x4x8 slice.
Arguments:
- act_in: bfloat16 [2, 32768, 1024], P(None, ('rep', 'fsdp')), parts along dimension 1
- grad_final: bfloat16 [2, 32768, 1024], P(None, ('rep', 'fsdp')), parts along dimension 1
- lengths: int32 [2, 16], P(None, ('rep', 'fsdp')), parts along dimension 1
- w_in: bfloat16 [2, 2048, 4096], P(None, ('rep', 'fsdp')), parts along dimension 1
- w_out: bfloat16 [2, 8192, 1024], P(None, ('rep', 'fsdp')), parts along dimension 1
Outputs:
- output 1: float32 [2, 2048, 4096], P(None, ('rep', 'fsdp')), parts along dimension 1
- output 2: float32 [2, 8192, 1024], P(None, ('rep', 'fsdp')), parts along dimension 1
There are 2 independent parts. The reference program is written for one: setup_inputs(seed, part) draws one part's arguments, and reference() takes and returns one part's arrays. A program takes and returns all parts, laid end to end along the dimension named above; each array names one.
All inputs are finite; a program needn't handle non-finite values.
Results may differ from the reference program's by a relative error of at most 0.00201851.
Values are sent between devices in bfloat16 or wider.
A program may use at most 768 MiB of HBM per device.

```python
import jax
import jax.numpy as jnp
from jax import lax

MICROBATCHES = 2
TOKENS_DEV = 2048
LAYERS = 2
D = 1024
FF = 4096
GROUP_SIZE = 8


def draw_lengths(key):
    num_slots = MICROBATCHES * GROUP_SIZE
    low_len = TOKENS_DEV // 4
    key_a, key_b, key_c = jax.random.split(key, 3)
    flat_lens = jax.random.randint(key_a, (num_slots,), low_len, TOKENS_DEV + 1)
    top_pos = jax.random.randint(key_b, (), 0, num_slots)
    low_pos = (top_pos + jax.random.randint(key_c, (), 1, num_slots)) % num_slots
    flat_lens = flat_lens.at[top_pos].set(TOKENS_DEV).at[low_pos].set(low_len)
    return flat_lens.reshape(MICROBATCHES, GROUP_SIZE).astype(jnp.int32)


def setup_inputs(seed: int = 0, part: int = 0) -> dict:
    part_key = jax.random.fold_in(jax.random.key(seed), part)
    key_list = jax.random.split(part_key, 5)
    group_rows = GROUP_SIZE * TOKENS_DEV
    grad_scale = (MICROBATCHES * group_rows) ** -0.5
    act_in = jax.random.normal(key_list[0], (MICROBATCHES, group_rows, D), jnp.float32)
    grad_final = jax.random.normal(key_list[1], (MICROBATCHES, group_rows, D), jnp.float32) * grad_scale
    w_in = jax.random.normal(key_list[2], (LAYERS, D, FF), jnp.float32) * D ** -0.5
    w_out = jax.random.normal(key_list[3], (LAYERS, FF, D), jnp.float32) * FF ** -0.5
    lengths = draw_lengths(key_list[4])
    return {"act_in": act_in.astype(jnp.bfloat16), "grad_final": grad_final.astype(jnp.bfloat16), "lengths": lengths, "w_in": w_in.astype(jnp.bfloat16), "w_out": w_out.astype(jnp.bfloat16)}


def gelu_back(pre_act, grad_act):
    _, pull_back = jax.vjp(lambda value_in: jax.nn.gelu(value_in, approximate=True), pre_act.astype(jnp.float32))
    return pull_back(grad_act)[0]


def block_grads(x_block, g_block, len_block, w_in, w_out):
    keep_row = jnp.arange(TOKENS_DEV)[:, None] < len_block

    def forward_layer(hidden, layer_w):
        w_layer_in, w_layer_out = layer_w
        pre_act = jnp.dot(hidden, w_layer_in, preferred_element_type=jnp.float32).astype(jnp.bfloat16)
        post_act = jax.nn.gelu(pre_act.astype(jnp.float32), approximate=True).astype(jnp.bfloat16)
        branch = jnp.dot(post_act, w_layer_out, preferred_element_type=jnp.float32)
        new_hidden = (hidden.astype(jnp.float32) + jnp.where(keep_row, branch, 0.0)).astype(jnp.bfloat16)
        return new_hidden, (hidden, pre_act, post_act)

    _, saved_acts = lax.scan(forward_layer, x_block, (w_in, w_out))

    def backward_layer(grad_x, layer_data):
        hidden, pre_act, post_act, w_layer_in, w_layer_out = layer_data
        grad_y = jnp.where(keep_row, grad_x, jnp.zeros_like(grad_x))
        grad_act = jnp.dot(grad_y, w_layer_out.T, preferred_element_type=jnp.float32)
        grad_pre = gelu_back(pre_act, grad_act).astype(jnp.bfloat16)
        part_out = jnp.dot(post_act.T, grad_y, preferred_element_type=jnp.float32)
        part_in = jnp.dot(hidden.T, grad_pre, preferred_element_type=jnp.float32)
        new_grad_x = (grad_x.astype(jnp.float32) + jnp.dot(grad_pre, w_layer_in.T, preferred_element_type=jnp.float32)).astype(jnp.bfloat16)
        return new_grad_x, (part_in, part_out)

    _, layer_grads = lax.scan(backward_layer, g_block, saved_acts + (w_in, w_out), reverse=True)
    return layer_grads


def reference(act_in, grad_final, lengths, w_in, w_out):
    num_blocks = MICROBATCHES * GROUP_SIZE
    x_blocks = act_in.reshape(num_blocks, TOKENS_DEV, D)
    g_blocks = grad_final.reshape(num_blocks, TOKENS_DEV, D)
    len_blocks = lengths.reshape(num_blocks)

    def accumulate(carry, block_data):
        acc_in, acc_out = carry
        part_in, part_out = block_grads(block_data[0], block_data[1], block_data[2], w_in, w_out)
        return (acc_in + part_in, acc_out + part_out), None

    init_acc = (jnp.zeros((LAYERS, D, FF), jnp.float32), jnp.zeros((LAYERS, FF, D), jnp.float32))
    (grad_w_in, grad_w_out), _ = lax.scan(accumulate, init_acc, (x_blocks, g_blocks, len_blocks))
    return grad_w_in, grad_w_out
```

```python
import jax
import jax.numpy as jnp
from jax import lax
from jax.experimental import pallas as pl
from jax.experimental.pallas import tpu as pltpu
from jax.sharding import PartitionSpec as P

CORES = 2
HB = 256
BM = 512
LW = 128
NTILES = 4
C0 = 0.7978845608028654
C1 = 0.044715
NT = (((1,), (1,)), ((), ()))
TN = (((0,), (0,)), ((), ()))
F32 = jnp.float32
BF16 = jnp.bfloat16

M_CORE, M_LEN = 1, 2


def params(*sem):
    return pltpu.CompilerParams(vmem_limit_bytes=60 * 1024 * 1024, dimension_semantics=sem)


def cost(flops, size, tr=0):
    return pl.CostEstimate(flops=flops, bytes_accessed=size, transcendentals=tr)


def half_tanh(h):
    h2 = h * h
    return h2, 0.5 + 0.5 * jnp.tanh(h * (C0 + (C0 * C1) * h2))


def gelu_slope(h, h2, e):
    return e + (h * (e * (1.0 - e))) * (2.0 * C0 + (6.0 * C0 * C1) * h2)


def step_row(i, m):
    return jnp.minimum(i, m[0] - 1)


def keep_rows(meta, i):
    r = lax.broadcasted_iota(jnp.int32, (BM, 1), 0)
    lim = jnp.where(r < HB, meta[M_LEN + 2 * i], meta[M_LEN + 2 * i + 1] + HB)
    return r < lim


def pack_rows(meta, own, peer, mask):
    rows, d = own.shape
    nb = rows // HB
    base = M_LEN + 2 * nb

    def hold(q, m):
        return q // nb * nb + jnp.minimum(lax.rem(q, nb), (BM // HB) * m[0] - 1)

    def body(meta, own_ref, peer_ref, o_ref):
        q = pl.program_id(0)
        src = meta[base + q]
        used = lax.rem(q, nb) < (BM // HB) * meta[0]

        def put(ref):
            v = ref[...]
            if mask:
                keep = lax.broadcasted_iota(jnp.int32, (HB, 1), 0) < meta[M_LEN + q]
                v = jnp.where(keep, v.astype(F32), 0.0).astype(BF16)
            o_ref[...] = v

        @pl.when(used & (src < nb))
        def _():
            put(own_ref)

        @pl.when(used & (src >= nb))
        def _():
            put(peer_ref)

    return pl.pallas_call(
        body, name="pack_rows",
        grid_spec=pltpu.PrefetchScalarGridSpec(
            num_scalar_prefetch=1, grid=(2 * nb,),
            in_specs=[
                pl.BlockSpec((HB, d), lambda q, m: (jnp.minimum(m[base + hold(q, m)], nb - 1), 0)),
                pl.BlockSpec((HB, d), lambda q, m: (jnp.maximum(m[base + hold(q, m)] - nb, 0), 0)),
            ],
            out_specs=pl.BlockSpec((HB, d), lambda q, m: (hold(q, m), 0))),
        out_shape=jax.ShapeDtypeStruct((2 * rows, d), own.dtype),
        compiler_params=params("arbitrary"), cost_estimate=cost(2 * rows * d, 8 * rows * d),
    )(meta, own, peer)


def fwd_h(meta, x, w, rows):
    d, f = w.shape
    half = f // CORES
    piece = NTILES * LW
    chips = half // piece

    def body(meta, x_ref, w_ref, hk_ref, hs_ref, a_ref):
        @pl.when(pl.program_id(0) < meta[0])
        def _():
            xb = x_ref[...]
            for r, h_ref in ((0, hk_ref), (1, hs_ref)):
                for c in range(chips):
                    col = pl.multiple_of((CORES * c + lax.rem(meta[M_CORE] + r, CORES)) * piece, piece)
                    hb = jnp.dot(xb, w_ref[:, pl.ds(col, piece)], preferred_element_type=F32).astype(BF16)
                    for n in range(NTILES):
                        h_ref[:, (n * chips + c) * LW:(n * chips + c + 1) * LW] = hb[:, n * LW:(n + 1) * LW]
                    hf = hb.astype(F32)
                    a_ref[:, pl.ds(col, piece)] = (hf * half_tanh(hf)[1]).astype(BF16)

    rb = lambda i, m: (step_row(i, m), 0)
    return pl.pallas_call(
        body, name="fwd_h",
        grid_spec=pltpu.PrefetchScalarGridSpec(
            num_scalar_prefetch=1, grid=(rows // BM,),
            in_specs=[pl.BlockSpec((BM, d), rb), pl.BlockSpec((d, f), lambda i, m: (0, 0))],
            out_specs=[pl.BlockSpec((BM, half), rb), pl.BlockSpec((BM, half), rb), pl.BlockSpec((BM, f), rb)]),
        out_shape=[jax.ShapeDtypeStruct((rows, half), BF16)] * 2 + [jax.ShapeDtypeStruct((rows, f), BF16)],
        compiler_params=params("arbitrary"), cost_estimate=cost(2 * rows * d * f, 2 * (rows * d + d * f + 2 * rows * f), rows * f),
    )(meta, x, w)


def fwd_half(meta, x_own, x_peer, w):
    rows, d = x_own.shape
    half = w.shape[1] // CORES
    piece = NTILES * LW
    chips = half // piece
    ns = rows // BM

    def body(meta, x0_ref, x1_ref, w_hbm, h0_ref, h1_ref, w_scr, sems):
        s, i = pl.program_id(0), pl.program_id(1)

        @pl.when((s == 0) & (i == 0))
        def _():
            copies = []
            for c in range(chips):
                at = pl.multiple_of((CORES * c + meta[M_CORE]) * piece, piece)
                copies.append(pltpu.make_async_copy(w_hbm.at[:, pl.ds(at, piece)], w_scr.at[:, pl.ds(c * piece, piece)], sems.at[c]))
            for cp in copies:
                cp.start()
            for cp in copies:
                cp.wait()

        for side, (x_ref, h_ref) in enumerate(((x0_ref, h0_ref), (x1_ref, h1_ref))):
            @pl.when((s == side) & (i < meta[0]))
            def _():
                xb = x_ref[...]
                for c in range(chips):
                    hb = jnp.dot(xb, w_scr[:, c * piece:(c + 1) * piece], preferred_element_type=F32).astype(BF16)
                    for n in range(NTILES):
                        h_ref[:, (n * chips + c) * LW:(n * chips + c + 1) * LW] = hb[:, n * LW:(n + 1) * LW]

    def spec(width, side):
        if side == 0:
            return pl.BlockSpec((BM, width), lambda s, i, m: (jnp.where(s == 0, step_row(i, m), m[0] - 1), 0))
        return pl.BlockSpec((BM, width), lambda s, i, m: (jnp.where(s == 1, step_row(i, m), 0), 0))

    return pl.pallas_call(
        body, name="fwd_half",
        grid_spec=pltpu.PrefetchScalarGridSpec(
            num_scalar_prefetch=1, grid=(2, ns),
            in_specs=[spec(d, 0), spec(d, 1), pl.BlockSpec(memory_space=pl.ANY)],
            out_specs=[spec(half, 0), spec(half, 1)],
            scratch_shapes=[pltpu.VMEM((d, half), BF16), pltpu.SemaphoreType.DMA((chips,))]),
        out_shape=[jax.ShapeDtypeStruct((rows, half), BF16)] * 2,
        compiler_params=params("arbitrary", "arbitrary"), cost_estimate=cost(4 * rows * d * half, 2 * (2 * rows * d + d * half + 2 * rows * half)),
    )(meta, x_own, x_peer, w)


def fwd_y(meta, x, a, w):
    rows, f = a.shape
    d = w.shape[1]
    cn = d // 2

    def body(meta, x_ref, a_ref, w_ref, o_ref):
        i = pl.program_id(0)

        @pl.when(i < meta[0])
        def _():
            keep = keep_rows(meta, i)
            for n in range(0, d, cn):
                y = jnp.dot(a_ref[...], w_ref[:, n:n + cn], preferred_element_type=F32)
                o_ref[:, n:n + cn] = (x_ref[:, n:n + cn].astype(F32) + jnp.where(keep, y, 0.0)).astype(BF16)

    rb = lambda i, m: (step_row(i, m), 0)
    return pl.pallas_call(
        body, name="fwd_y",
        grid_spec=pltpu.PrefetchScalarGridSpec(
            num_scalar_prefetch=1, grid=(rows // BM,),
            in_specs=[pl.BlockSpec((BM, d), rb), pl.BlockSpec((BM, f), rb), pl.BlockSpec((f, d), lambda i, m: (0, 0))],
            out_specs=pl.BlockSpec((BM, d), rb)),
        out_shape=jax.ShapeDtypeStruct((rows, d), BF16),
        compiler_params=params("arbitrary"), cost_estimate=cost(2 * rows * d * f, 2 * (2 * rows * d + d * f + rows * f)),
    )(meta, x, a, w)


def layer_tile(meta, n, xs, dys, hs, w1, w2, want_dh):
    d, f = w1.shape
    rows = xs[2]
    chips = f // (CORES * NTILES * LW)
    tw = chips * LW
    big = 2 * BM
    ns = rows // big
    npeer = d // (CORES * chips)
    have_h = hs is not None
    x_two, dy_two = xs[0][0] is not xs[0][1], dys[0][0] is not dys[0][1]

    def body(meta, *refs):
        refs = list(refs)
        x_refs = [refs.pop(0), refs.pop(0)] if x_two else [refs.pop(0)] * 2
        dy_refs = [refs.pop(0), refs.pop(0)] if dy_two else [refs.pop(0)] * 2
        h_refs = [refs.pop(0), refs.pop(0)] if have_h else None
        w1_hbm = None if have_h else refs.pop(0)
        w2_hbm = refs.pop(0)
        g_ref = refs.pop(0)
        dh_refs = [refs.pop(0), refs.pop(0)] if want_dh else None
        w1_scr = None if have_h else refs.pop(0)
        w2_scr, a1_scr, a2_scr, sems = refs
        s, i = pl.program_id(0), pl.program_id(1)

        @pl.when((s == 0) & (i == 0))
        def _():
            copies = []
            for c in range(chips):
                at = pl.multiple_of(((CORES * c + meta[M_CORE]) * NTILES + n) * LW, LW)
                if not have_h:
                    copies.append(pltpu.make_async_copy(w1_hbm.at[:, pl.ds(at, LW)], w1_scr.at[:, pl.ds(c * LW, LW)], sems.at[2 * c]))
                copies.append(pltpu.make_async_copy(w2_hbm.at[pl.ds(at, LW), :], w2_scr.at[pl.ds(c * LW, LW), :], sems.at[2 * c + 1]))
            for cp in copies:
                cp.start()
            a1_scr[...] = jnp.zeros_like(a1_scr)
            a2_scr[...] = jnp.zeros_like(a2_scr)
            for cp in copies:
                cp.wait()

        def work(side, lo, m):
            x, dy = x_refs[side][lo:lo + m, :], dy_refs[side][lo:lo + m, :]
            if have_h:
                hb = h_refs[side][lo:lo + m, :]
            else:
                hb = jnp.dot(x, w1_scr[...], preferred_element_type=F32).astype(BF16)
            da = lax.dot_general(dy, w2_scr[...], NT, preferred_element_type=F32)
            h = hb.astype(F32)
            h2, e = half_tanh(h)
            act = (h * e).astype(BF16)
            dh = (gelu_slope(h, h2, e) * da).astype(BF16)
            if want_dh:
                dh_refs[side][lo:lo + m, :] = dh
            a2_scr[...] += lax.dot_general(act, dy, TN, preferred_element_type=F32)
            a1_scr[...] += lax.dot_general(x, dh, TN, preferred_element_type=F32)

        for side in range(2):
            @pl.when((s == side) & (2 * i + 1 < meta[0]))
            def _():
                work(side, 0, big)

            @pl.when((s == side) & (2 * i + 1 == meta[0]))
            def _():
                work(side, 0, BM)

        @pl.when((s == 1) & (i == ns - 1))
        def _():
            for c in range(chips):
                g_ref[c, 0:LW, :] = a2_scr[c * LW:(c + 1) * LW, :]
                for r in range(CORES):
                    at = pl.multiple_of((CORES * c + lax.rem(meta[M_CORE] + r, CORES)) * npeer, npeer)
                    g_ref[c, LW:2 * LW, r * tw:(r + 1) * tw] = a1_scr[pl.ds(at, npeer), :]

    def rowspec(width, first, side, col=0):
        def im(s, i, m):
            last = (m[0] + 1) // 2 - 1
            cur = jnp.minimum(i, last) if side == 1 else jnp.where(s == 0, jnp.minimum(i, last), last)
            cur = cur if side == 0 else jnp.where(s == 1, cur, 0)
            return (first + cur, col)
        return pl.BlockSpec((big, width), im)

    def bothspec(first):
        return pl.BlockSpec((big, d), lambda s, i, m: (first * s + jnp.minimum(i, (m[0] + 1) // 2 - 1), 0))

    in_specs, args = [], []
    for (two, v) in ((x_two, xs), (dy_two, dys)):
        in_specs += [rowspec(d, v[1][k], k) for k in range(2)] if two else [bothspec(v[1][1])]
        args += list(v[0]) if two else [v[0][0]]
    if have_h:
        in_specs += [rowspec(tw, 0, k, n) for k in range(2)]
        args += list(hs)
    else:
        in_specs += [pl.BlockSpec(memory_space=pl.ANY)]
        args += [w1]
    in_specs += [pl.BlockSpec(memory_space=pl.ANY)]
    args += [w2]
    out_specs = [pl.BlockSpec((chips, 2 * LW, d), lambda s, i, m: (0, 0, 0))]
    out_shape = [jax.ShapeDtypeStruct((chips, 2 * LW, d), F32)]
    if want_dh:
        out_specs += [rowspec(tw, 0, 0), rowspec(tw, 0, 1)]
        out_shape += [jax.ShapeDtypeStruct((rows, tw), BF16)] * 2
    scratch = [] if have_h else [pltpu.VMEM((d, tw), BF16)]
    scratch += [pltpu.VMEM((tw, d), BF16), pltpu.VMEM((d, tw), F32), pltpu.VMEM((tw, d), F32), pltpu.SemaphoreType.DMA((2 * chips,))]
    mm = 3 if have_h else 4
    return pl.pallas_call(
        body, name=f"layer_tile_{'l' if have_h else 'u'}",
        grid_spec=pltpu.PrefetchScalarGridSpec(num_scalar_prefetch=1, grid=(2, ns), in_specs=in_specs, out_specs=out_specs, scratch_shapes=scratch),
        out_shape=out_shape,
        compiler_params=params("arbitrary", "arbitrary"),
        cost_estimate=cost(2 * mm * 2 * rows * d * tw, 2 * (4 * rows * d + 2 * d * tw + 2 * rows * tw) + 8 * d * tw, 2 * rows * tw),
    )(meta, *args)


def bwd_x(meta, dy, dhs, w):
    d, f = w.shape
    rows = dhs[0].shape[0]
    tw = dhs[0].shape[1]
    chips = tw // LW
    cn = d // 2

    def body(meta, dy_ref, *refs):
        dh_refs, w_ref, o_ref, w_scr = refs[:len(dhs)], refs[len(dhs)], refs[-2], refs[-1]
        i = pl.program_id(0)

        @pl.when(i == 0)
        def _():
            for r in range(CORES):
                core = lax.rem(meta[M_CORE] + r, CORES)
                for n in range(NTILES):
                    for c in range(chips):
                        col = pl.multiple_of(((CORES * c + core) * NTILES + n) * LW, LW)
                        to = ((r * NTILES + n) * chips + c) * LW
                        w_scr[:, to:to + LW] = w_ref[:, pl.ds(col, LW)]

        @pl.when(i < meta[0])
        def _():
            keep = keep_rows(meta, i)
            dh = jnp.concatenate([r[...] for r in dh_refs], axis=1)
            for n in range(0, d, cn):
                u = lax.dot_general(dh, w_scr[n:n + cn, :], NT, preferred_element_type=F32)
                o_ref[:, n:n + cn] = jnp.where(keep, dy_ref[:, n:n + cn].astype(F32) + u, 0.0).astype(BF16)

    rb = lambda i, m: (step_row(i, m), 0)
    return pl.pallas_call(
        body, name="bwd_x",
        grid_spec=pltpu.PrefetchScalarGridSpec(
            num_scalar_prefetch=1, grid=(rows // BM,),
            in_specs=[pl.BlockSpec((BM, d), rb)] + [pl.BlockSpec((BM, tw), rb)] * len(dhs) + [pl.BlockSpec((d, f), lambda i, m: (0, 0))],
            out_specs=pl.BlockSpec((BM, d), rb), scratch_shapes=[pltpu.VMEM((d, f), BF16)]),
        out_shape=jax.ShapeDtypeStruct((rows, d), BF16),
        compiler_params=params("arbitrary"), cost_estimate=cost(2 * rows * d * f, 2 * (2 * rows * d + d * f + rows * f)),
    )(meta, dy, *dhs, w)


def finish(meta, l, tiles, got, prev, num_layers):
    tw = got[0].shape[1]
    d = tiles[0].shape[1]
    chips = tw // LW
    nt = len(tiles)

    def body(meta, *refs):
        t_refs, p_refs, oi_ref, oo_ref = refs[:nt], refs[nt:2 * nt], refs[-2], refs[-1]
        for n in range(nt):
            oo_ref[0, n * LW:(n + 1) * LW, :] = t_refs[n][0:LW, :]
            for c in range(chips):
                for r in range(CORES):
                    at = pl.multiple_of(((CORES * c + lax.rem(meta[M_CORE] + r, CORES)) * nt + n) * LW, LW)
                    v = t_refs[n][LW:2 * LW, c * LW:(c + 1) * LW] if r == 0 else p_refs[n][:, c * LW:(c + 1) * LW]
                    oi_ref[0, :, pl.ds(at, LW)] = v

    whole = lambda shape: pl.BlockSpec(shape, lambda i, m: (0, 0))
    in_specs = [whole((2 * LW, d))] * nt + [whole((LW, tw))] * nt
    args = list(tiles) + list(got)
    alias = {}
    if prev is not None:
        in_specs += [pl.BlockSpec(memory_space=pl.ANY)] * 2
        args += list(prev)
        alias = {1 + 2 * nt: 0, 2 + 2 * nt: 1}
    return pl.pallas_call(
        body, name="finish",
        grid_spec=pltpu.PrefetchScalarGridSpec(
            num_scalar_prefetch=1, grid=(1,), in_specs=in_specs,
            out_specs=[pl.BlockSpec((1, LW, CORES * nt * tw), lambda i, m: (l, 0, 0)), pl.BlockSpec((1, nt * LW, d), lambda i, m: (l, 0, 0))]),
        out_shape=[jax.ShapeDtypeStruct((num_layers, LW, CORES * nt * tw), F32), jax.ShapeDtypeStruct((num_layers, nt * LW, d), F32)],
        input_output_aliases=alias,
        compiler_params=params("arbitrary"), cost_estimate=cost(1 << 28, 20 * LW * nt * d),
    )(meta, *args)


def row_plan(lens_pair, core, blocks_dev):
    nb = CORES * blocks_dev
    b = jnp.arange(nb)
    seg = lens_pair[b // (blocks_dev // lens_pair.shape[1] * lens_pair.shape[1]), (b % blocks_dev) // (blocks_dev // lens_pair.shape[1])]
    per = blocks_dev // lens_pair.shape[1]
    real = jnp.clip(seg - HB * (b % per), 0, HB)
    live = (real > 0).astype(jnp.int32)
    n_live = jnp.sum(live)
    pos = jnp.where(live > 0, jnp.cumsum(live) - 1, n_live + jnp.cumsum(1 - live) - 1)
    q = jnp.arange(nb)
    want = jnp.where(q < blocks_dev, CORES * q + core, CORES * (q - blocks_dev) + 1 - core)
    hit = (pos[None, :] == want[:, None]).astype(jnp.int32)
    src = jnp.sum(hit * b[None, :], axis=1)
    cnt = jnp.sum(hit * real[None, :], axis=1)
    src = jnp.where((src // blocks_dev) == core, src % blocks_dev, blocks_dev + src % blocks_dev)
    per_step = CORES * (BM // HB)
    steps = (n_live + per_step - 1) // per_step
    return jnp.concatenate([steps[None], core[None], cnt, src]).astype(jnp.int32)


def solution(mesh):
    row_spec = P(None, ("rep", "fsdp"), None)
    len_spec = P(None, ("rep", "fsdp"))
    nd = mesh.shape["fsdp"]
    chips = nd // CORES
    swap = [(j, j ^ 1) for j in range(nd)]
    rings = [[CORES * c + k for c in range(chips)] for k in range(CORES)]

    def peer(v):
        return lax.ppermute(v, "fsdp", swap)

    def local_grads(act_in, grad_final, lengths, w_in, w_out):
        num_layers = w_in.shape[0]
        d = act_in.shape[2]
        rows = act_in.shape[0] * act_in.shape[1]
        ns = rows // BM
        core = lax.rem(lax.axis_index("fsdp"), CORES)
        x_own = act_in.reshape(rows, d)
        g_own = grad_final.reshape(rows, d)
        len_own = lengths[:, 0]
        len_peer = peer(len_own)
        x_peer = peer(x_own)
        full = []
        for l in range(num_layers):
            full.append((lax.all_gather(w_in[l], "fsdp", axis=0, tiled=True), lax.all_gather(w_out[l], "fsdp", axis=0, tiled=True)))
        g_peer = peer(g_own)
        lens_pair = jnp.where(core == 0, jnp.stack([len_own, len_peer]), jnp.stack([len_peer, len_own]))
        meta = row_plan(lens_pair, core, rows // HB)
        x_pair = pack_rows(meta, x_own, x_peer, False)
        g_pair = pack_rows(meta, g_own, g_peer, True)

        saved = []
        x_cur = ((x_pair, x_pair), (0, ns // 2), rows)
        for l in range(num_layers - 1):
            h_keep, h_send, act = fwd_h(meta, x_cur[0][0], full[l][0], rows)
            saved.append((x_cur, (h_keep, peer(h_send))))
            x_next = fwd_y(meta, x_cur[0][0], act, full[l][1])
            x_cur = ((x_next, peer(x_next)), (0, 0), rows)
        saved.append((x_cur, fwd_half(meta, x_cur[0][0], x_cur[0][1], full[-1][0])))

        dy_cur = ((g_pair, g_pair), (0, ns // 2))
        outs = None
        tw = d // CORES
        for l in reversed(range(num_layers)):
            xs, hs = saved[l]
            own, got, tiles, swapped = [], [], [], []
            for n in range(NTILES):
                if l + 1 < num_layers and n == NTILES - 1:
                    meta, outs = lax.optimization_barrier((meta, outs))
                res = layer_tile(meta, n, xs, dy_cur, hs, full[l][0], full[l][1], l > 0)
                if l > 0:
                    own.append(res[1])
                    got.append(peer(res[2]))
                t = lax.psum_scatter(res[0], "fsdp", scatter_dimension=0, axis_index_groups=rings, tiled=True)[0]
                tiles.append(t)
                swapped.append(peer(t[LW:, tw:]))
            if l > 0:
                dy_new = bwd_x(meta, dy_cur[0][0], own + got, full[l][0])
                dy_cur = ((dy_new, peer(dy_new)), (0, 0))
            outs = finish(meta, l, tiles, swapped, outs, num_layers)
        return tuple(outs)

    return jax.shard_map(local_grads, mesh=mesh, in_specs=(row_spec, row_spec, len_spec, row_spec, row_spec), out_specs=(row_spec, row_spec), check_vma=False)
```
